32 devices in a mesh: groups: 2 (over x), rows: 16 (over z, y, core).
Axes of the slice: x: 2, y: 2, z: 4, core: 2. Of those that a mesh axis runs over, the one named last changes fastest.
Arguments:
- slide_band: bfloat16 [96, 256, 512], P(None, ('groups', 'rows')), parts along dimension 1, may hold values from -8 to 8
- tissue_flags: int32 [32, 64], P(('groups', 'rows')), parts along dimension 0, may hold values from 0 to 1, as said below
- stain_index: int32 [32, 64], P(('groups', 'rows')), parts along dimension 0, may hold values from 0 to 3
- stain_gain: float32 [4, 96], replicated, may hold values from 0.5 to 2
- conv_weights: bfloat16 [3, 9, 96, 96], replicated, may hold values from -0.21875 to 0.21875
- norm_gain: float32 [3, 96], replicated, may hold values from 0.5 to 2
- norm_bias: float32 [3, 96], replicated, may hold values from -3 to 3
Outputs:
- features: bfloat16 [96, 256, 512], P(None, ('groups', 'rows')), parts along dimension 1
The draws below stay inside these ranges and needn't reach their ends.
There are 2 independent parts, one for each index of `groups`. The reference program is written for one: setup_inputs(seed, part) draws one part's arguments, and reference() takes and returns one part's arrays. A program takes and returns all parts, laid end to end along the dimension named above; an argument that names none is the same for every part. Nothing has to cross between parts.
Inputs may be any that keep to these rules, and one draw needn't show every extreme that they name: `tissue_flags`: in every aligned block of 1 tile rows, the first tile of the block's first tile row is tissue.
All inputs are finite; a program needn't handle non-finite values.
Results may differ from the reference program's by a relative error of at most 0.018.
Values may be sent and summed in bfloat16 or wider, within the bound.
A program may use at most 64 MiB of HBM per device.

```python
import math
import jax
import jax.numpy as jnp
from jax import lax

CHANNELS = 96
LAYERS = 3
TILE = 8
STAINS = 4
BAND_ROWS = 8
COLUMNS = 512
HEIGHT = 128


def draw_slide_band(key, part):
    first_key = jax.random.fold_in(jax.random.fold_in(key, 11), 0)
    position = jnp.arange(HEIGHT, dtype=jnp.float32) / max(HEIGHT - 1, 1)
    base = jax.random.normal(first_key, (CHANNELS, HEIGHT, COLUMNS), jnp.float32)
    values = base * (0.6 + 1.2 * position)[None, :, None]
    return jnp.clip(values, -8.0, 8.0).astype(jnp.bfloat16)


def draw_tissue_flags(key, part):
    tile_rows = HEIGHT // TILE
    tile_cols = COLUMNS // TILE
    rolled = jax.random.randint(jax.random.fold_in(key, 23), (tile_rows, tile_cols), 0, 1000)
    row_ids = jnp.arange(tile_rows, dtype=jnp.int32)[:, None]
    col_ids = jnp.arange(tile_cols, dtype=jnp.int32)[None, :]
    threshold = 250 + 700 * row_ids // max(tile_rows - 1, 1)
    flags = (rolled < threshold).astype(jnp.int32)
    block_rows = BAND_ROWS // TILE
    forced = (row_ids % block_rows == 0) & (col_ids == 0)
    return jnp.where(forced, 1, flags).astype(jnp.int32)


def plant(values, key, low, largest):
    extent = values.shape
    index_at = [jax.random.randint(jax.random.fold_in(key, axis), (), 0, extent[axis]) for axis in range(len(extent))]
    values = values.at[tuple(index_at)].set(low)
    longest = extent.index(max(extent))
    index_at[longest] = (index_at[longest] + 1) % extent[longest]
    return values.at[tuple(index_at)].set(largest)


def gaussian(own_key, extent, spread, limit, kind=jnp.bfloat16):
    return jnp.clip(spread * jax.random.normal(own_key, extent, jnp.float32), -limit, limit).astype(kind)


def setup_inputs(seed: int = 0, part: int = 0) -> dict:
    key_list = jax.random.split(jax.random.key(seed), 8)
    own_keys = jax.random.split(jax.random.fold_in(key_list[7], part), 8)
    return {
        "slide_band": draw_slide_band(jax.random.fold_in(jax.random.fold_in(key_list[7], part), 71), part),
        "tissue_flags": draw_tissue_flags(jax.random.fold_in(jax.random.fold_in(key_list[7], part), 71), part),
        "stain_index": plant(jax.random.randint(own_keys[2], (HEIGHT // TILE, COLUMNS // TILE), 0, STAINS), jax.random.fold_in(own_keys[2], 1), 0, STAINS - 1).astype(jnp.int32),
        "stain_gain": jnp.clip(jnp.exp(jax.random.uniform(key_list[3], (STAINS, CHANNELS), jnp.float32, math.log(0.5), math.log(2.0))), 0.5, 2.0),
        "conv_weights": gaussian(key_list[4], (LAYERS, 9, CHANNELS, CHANNELS), (9 * CHANNELS) ** -0.5, 0.21875),
        "norm_gain": jnp.clip(jnp.exp(jax.random.uniform(key_list[5], (LAYERS, CHANNELS), jnp.float32, math.log(0.5), math.log(2.0))), 0.5, 2.0),
        "norm_bias": gaussian(key_list[6], (LAYERS, CHANNELS), 0.5, 3.0, jnp.float32),
    }


epsilon = 1e-05

def spread_tiles(tiles):
    return jnp.repeat(jnp.repeat(tiles, TILE, axis=-2), TILE, axis=-1)

def conv_layer(inputs, weights, spacing):
    height = inputs.shape[1]
    col_count = inputs.shape[2]
    padded = jnp.pad(inputs, ((0, 0), (spacing, spacing), (spacing, spacing)))
    running = jnp.zeros((weights.shape[1], height, col_count), jnp.float32)
    for kernel_tap in range(9):
        row_tap = kernel_tap // 3
        col_tap = kernel_tap % 3
        window = padded[:, row_tap * spacing:row_tap * spacing + height, col_tap * spacing:col_tap * spacing + col_count]
        running = running + jnp.einsum('oc,chw->ohw', weights[kernel_tap].astype(jnp.float32), window)
    return running

def reference(slide_band, tissue_flags, stain_index, stain_gain, conv_weights, norm_gain, norm_bias):
    pixels = spread_tiles(tissue_flags.astype(jnp.float32))
    stain_scale = spread_tiles(jnp.transpose(stain_gain[stain_index], (2, 0, 1)))
    current = (slide_band.astype(jnp.float32) * stain_scale * pixels[None]).astype(jnp.bfloat16)
    count_all = jnp.sum(pixels)
    for layer_index in range(LAYERS):
        spacing = 2 ** layer_index
        response = conv_layer(current.astype(jnp.float32), conv_weights[layer_index], spacing)
        average = lax.optimization_barrier(jnp.sum(response * pixels[None], axis=(1, 2))) / count_all
        centred = response - average[:, None, None]
        variance = lax.optimization_barrier(jnp.sum(centred * centred * pixels[None], axis=(1, 2))) / count_all
        scaled = norm_gain[layer_index][:, None, None] * centred * lax.rsqrt(variance + epsilon)[:, None, None] + norm_bias[layer_index][:, None, None]
        current = (jnp.maximum(scaled, 0.0) * pixels[None]).astype(jnp.bfloat16)
    return current
```

```python
import functools

import jax
import jax.numpy as jnp
from jax import lax
from jax.experimental import pallas as pl
from jax.experimental.pallas import tpu as pltpu
from jax.sharding import PartitionSpec as P

LAYERS = 3
TILE = 8
STAINS = 4
REACH = 2**LAYERS - 1
EPSILON = 1e-05
MESH = pl.DeviceIdType.MESH


def kernel(
    peers,
    slide_ref,
    flags_ref,
    index_ref,
    stain_ref,
    weights_ref,
    gain_ref,
    bias_ref,
    out_ref,
    turned,
    x0,
    x1,
    x2,
    response,
    taps,
    masks,
    flag_out,
    flag_in,
    tally_out,
    tally_in,
    edge_send,
    edge_recv,
    tally_send,
    tally_recv,
):
    channels, rows, cols = slide_ref.shape
    tiles = flags_ref.shape[1]
    me = lax.axis_index("rows")
    has_up = me > 0
    has_down = me < peers - 1
    inputs = (x0, x1, x2)
    first = (REACH, REACH - 1, REACH - 3)
    base = REACH - 1

    flag_in[...] = jnp.zeros_like(flag_in)
    barrier = pltpu.get_barrier_semaphore()

    def greet(step, carry):
        other = lax.rem(me + step, peers)
        pl.semaphore_signal(barrier, inc=1, device_id={"rows": other}, device_id_type=MESH)
        return carry

    lax.fori_loop(1, peers, greet, 0)

    spread = (
        lax.broadcasted_iota(jnp.int32, (128, cols), 1) // TILE
        == lax.broadcasted_iota(jnp.int32, (128, cols), 0)
    ).astype(jnp.float32)
    eye = lax.broadcasted_iota(jnp.int32, (channels, channels), 0) == lax.broadcasted_iota(
        jnp.int32, (channels, channels), 1
    )

    def column(row):
        return jnp.sum(jnp.where(eye, row, 0.0), axis=1, keepdims=True)

    def as_row(col):
        return jnp.sum(jnp.where(eye, col, 0.0), axis=0, keepdims=True)

    def widen(flags):
        return jnp.dot(flags, spread, preferred_element_type=jnp.float32)

    flag_out[...] = jnp.zeros_like(flag_out)
    flag_out[:, 0:tiles] = jnp.broadcast_to(
        flags_ref[...].astype(jnp.float32), (flag_out.shape[0], tiles)
    )
    masks[0] = widen(flag_out[...])
    classes = jnp.dot(
        jnp.broadcast_to(index_ref[...].astype(jnp.float32), (8, tiles)),
        spread[0:tiles],
        preferred_element_type=jnp.float32,
    )[0:1]
    scale = jnp.zeros((channels, cols), jnp.float32)
    for stain in range(STAINS):
        scale = jnp.where(classes == stain, column(stain_ref[stain : stain + 1, :]), scale)

    chunks = cols // 128
    for at in range(chunks):
        turned[at] = (
            slide_ref[:, :, at * 128 : (at + 1) * 128]
            .astype(jnp.float32)
            .reshape(channels * rows, 128)
        )
    response[0] = scale
    lane = lax.broadcasted_iota(jnp.int32, (1, cols), 1)

    def place(buffer, row, values, spacing):
        buffer[1, row] = values.astype(jnp.bfloat16)
        shifted = pltpu.roll(values, spacing, 1)
        buffer[0, row] = jnp.where(lane >= spacing, shifted, 0.0).astype(jnp.bfloat16)
        shifted = pltpu.roll(values, cols - spacing, 1)
        buffer[2, row] = jnp.where(lane < cols - spacing, shifted, 0.0).astype(jnp.bfloat16)

    def load_row(row, carry):
        values = jnp.concatenate(
            [turned[at, pl.ds(row, channels, stride=rows), :] for at in range(chunks)], axis=1
        )
        values = values * response[0] * masks[0, 0:1, :]
        values = values.astype(jnp.bfloat16).astype(jnp.float32)
        place(x0, first[0] + row, values, 1)
        return carry

    lax.fori_loop(0, rows, load_row, 0)

    @pl.when(jnp.logical_not(has_up))
    def _():
        x0[1, 0:REACH] = jnp.zeros((REACH, channels, cols), jnp.bfloat16)

    @pl.when(jnp.logical_not(has_down))
    def _():
        x0[1, REACH + rows : 2 * REACH + rows] = jnp.zeros((REACH, channels, cols), jnp.bfloat16)

    pl.semaphore_wait(barrier, peers - 1)

    def edge_copy(piece, side):
        if piece == 0:
            source, target = flag_out, flag_in.at[1 - side]
        else:
            lo, count = 2 ** (piece - 1) - 1, 2 ** (piece - 1)
            if side == 0:
                start, land = REACH + lo, REACH + rows + lo
            else:
                start, land = REACH + rows - lo - count, REACH - lo - count
            source, target = x0.at[1, pl.ds(start, count)], x0.at[1, pl.ds(land, count)]
        return pltpu.make_async_remote_copy(
            src_ref=source,
            dst_ref=target,
            send_sem=edge_send.at[piece, side],
            recv_sem=edge_recv.at[piece, side],
            device_id={"rows": me - 1 if side == 0 else me + 1},
            device_id_type=MESH,
        )

    def send_edge(piece):
        @pl.when(has_up)
        def _():
            edge_copy(piece, 0).start()

        @pl.when(has_down)
        def _():
            edge_copy(piece, 1).start()

    def take_edge(piece):
        @pl.when(has_down)
        def _():
            edge_copy(piece, 0).wait_recv()

        @pl.when(has_up)
        def _():
            edge_copy(piece, 1).wait_recv()

    for piece in (1, 0, 2, 3):
        send_edge(piece)

    for layer in range(LAYERS):
        for tap in range(9):
            taps[layer, :, tap * channels : (tap + 1) * channels] = weights_ref[layer, tap]

    def widen_edge(piece):
        lo, count = 2 ** (piece - 1) - 1, 2 ** (piece - 1)
        for start in (REACH - lo - count, REACH + rows + lo):
            def one(row, carry):
                place_shifts(x0, start + row)
                return carry
            lax.fori_loop(0, count, one, 0)

    def place_shifts(buffer, row):
        values = buffer[1, row].astype(jnp.float32)
        shifted = pltpu.roll(values, 1, 1)
        buffer[0, row] = jnp.where(lane >= 1, shifted, 0.0).astype(jnp.bfloat16)
        shifted = pltpu.roll(values, cols - 1, 1)
        buffer[2, row] = jnp.where(lane < cols - 1, shifted, 0.0).astype(jnp.bfloat16)

    def conv_row(layer, row):
        spacing = 2**layer
        source = inputs[layer]
        window = jnp.concatenate(
            [
                source[b, first[layer] + row + (a - 1) * spacing]
                for a in range(3)
                for b in range(3)
            ],
            axis=0,
        )
        return jnp.dot(taps[layer], window, preferred_element_type=jnp.float32)

    def conv_edges(layer, lo, count):
        for start in (-lo - count, rows + lo):
            def one(row, carry):
                response[base + start + row] = conv_row(layer, start + row)
                return carry
            lax.fori_loop(0, count, one, 0)

    def fold(values):
        total = values[:, 0:128]
        for at in range(128, cols, 128):
            total = total + values[:, at : at + 128]
        return total

    def conv_own(layer):
        def one(row, carry):
            sums, squares = carry
            own = conv_row(layer, row)
            response[base + row] = own
            masked = own * masks[0, 0:1, :]
            return sums + fold(masked), squares + fold(masked * own)

        zero = jnp.zeros((channels, 128), jnp.float32)
        sums, squares = lax.fori_loop(0, rows, one, (zero, zero))
        tally_out[layer] = jnp.zeros(tally_out.shape[1:], jnp.float32)
        tally_out[layer, 0:1, 0:channels] = as_row(jnp.sum(sums, axis=1, keepdims=True))
        tally_out[layer, 1:2, 0:channels] = as_row(jnp.sum(squares, axis=1, keepdims=True))
        pixels = jnp.sum(masks[0, 0:1, :], axis=1, keepdims=True) * rows
        tally_out[layer, 2:3, :] = jnp.broadcast_to(pixels, (1, 128))
        tally_in[layer, me] = tally_out[layer]

    def tally_copy(layer, step, other, slot):
        return pltpu.make_async_remote_copy(
            src_ref=tally_out.at[layer],
            dst_ref=tally_in.at[layer, slot],
            send_sem=tally_send.at[layer, step],
            recv_sem=tally_recv.at[layer, slot],
            device_id={"rows": other},
            device_id_type=MESH,
        )

    def send_tally(layer):
        def one(step, carry):
            tally_copy(layer, step, lax.rem(me + step, peers), me).start()
            return carry

        lax.fori_loop(1, peers, one, 0)

    def take_tally(layer):
        def one(step, carry):
            other = lax.rem(me + step, peers)
            tally_copy(layer, step, other, other).wait_recv()
            return carry

        lax.fori_loop(1, peers, one, 0)
        total = jnp.sum(tally_in[layer], axis=0)
        count = total[2:3, 0:channels]
        average = total[0:1, 0:channels] / count
        variance = jnp.maximum(total[1:2, 0:channels] / count - average * average, 0.0)
        factor = gain_ref[layer : layer + 1, :] * lax.rsqrt(variance + EPSILON)
        return column(average), column(factor), column(bias_ref[layer : layer + 1, :])

    def finish_row(row, norm, mask):
        average, factor, bias = norm
        scaled = (response[base + row] - average) * factor + bias
        return jnp.maximum(scaled, 0.0) * masks[mask, 0:1, :]

    def finish(layer, start, count, norm, mask):
        def one(row, carry):
            place(
                inputs[layer + 1],
                first[layer + 1] + start + row,
                finish_row(start + row, norm, mask),
                2 ** (layer + 1),
            )
            return carry

        lax.fori_loop(0, count, one, 0)

    def finish_edges(layer, lo, count, norm):
        finish(layer, -lo - count, count, norm, 1)
        finish(layer, rows + lo, count, norm, 2)

    take_edge(1)
    widen_edge(1)
    conv_own(0)
    send_tally(0)
    take_edge(0)
    masks[1] = widen(flag_in[0])
    masks[2] = widen(flag_in[1])
    take_edge(2)
    widen_edge(2)
    conv_edges(0, 0, 2)
    norm0 = take_tally(0)
    finish(0, 0, rows, norm0, 0)
    finish_edges(0, 0, 2, norm0)
    take_edge(3)
    widen_edge(3)
    conv_edges(0, 2, 4)
    finish_edges(0, 2, 4, norm0)
    conv_own(1)
    send_tally(1)
    conv_edges(1, 0, 4)
    norm1 = take_tally(1)
    finish(1, 0, rows, norm1, 0)
    finish_edges(1, 0, 4, norm1)
    conv_own(2)
    send_tally(2)
    norm2 = take_tally(2)

    def last(row, carry):
        values = finish_row(row, norm2, 0)
        for at in range(chunks):
            turned[at, pl.ds(row, channels, stride=rows), :] = values[:, at * 128 : (at + 1) * 128]
        return carry

    lax.fori_loop(0, rows, last, 0)
    for at in range(chunks):
        out_ref[:, :, at * 128 : (at + 1) * 128] = (
            turned[at].reshape(channels, rows, 128).astype(out_ref.dtype)
        )

    for piece in range(4):
        @pl.when(has_up)
        def _():
            edge_copy(piece, 0).wait_send()

        @pl.when(has_down)
        def _():
            edge_copy(piece, 1).wait_send()

    for layer in range(LAYERS):
        def one(step, carry):
            tally_copy(layer, step, lax.rem(me + step, peers), me).wait_send()
            return carry

        lax.fori_loop(1, peers, one, 0)


def per_device(peers, *arrays):
    channels, rows, cols = arrays[0].shape
    assert rows == TILE and rows > REACH and arrays[1].shape[0] == 1
    f32, bf16 = jnp.float32, jnp.bfloat16
    vmem = pl.BlockSpec(memory_space=pltpu.VMEM)
    return pl.pallas_call(
        functools.partial(kernel, peers),
        out_shape=jax.ShapeDtypeStruct((channels, rows, cols), bf16),
        in_specs=[vmem] * 7,
        out_specs=vmem,
        scratch_shapes=[
            pltpu.VMEM((cols // 128, channels * rows, 128), f32),
            pltpu.VMEM((3, rows + 2 * REACH, channels, cols), bf16),
            pltpu.VMEM((3, rows + 2 * (REACH - 1), channels, cols), bf16),
            pltpu.VMEM((3, rows + 2 * (REACH - 3), channels, cols), bf16),
            pltpu.VMEM((rows + 2 * (REACH - 1), channels, cols), f32),
            pltpu.VMEM((LAYERS, channels, 9 * channels), bf16),
            pltpu.VMEM((3, 8, cols), f32),
            pltpu.VMEM((8, 128), f32),
            pltpu.VMEM((2, 8, 128), f32),
            pltpu.VMEM((LAYERS, 8, 128), f32),
            pltpu.VMEM((LAYERS, peers, 8, 128), f32),
            pltpu.SemaphoreType.DMA((4, 2)),
            pltpu.SemaphoreType.DMA((4, 2)),
            pltpu.SemaphoreType.DMA((LAYERS, peers)),
            pltpu.SemaphoreType.DMA((LAYERS, peers)),
        ],
        compiler_params=pltpu.CompilerParams(
            collective_id=0, has_side_effects=True, vmem_limit_bytes=56 * 2**20
        ),
    )(*arrays)


def solution(mesh):
    banded = P(None, ("groups", "rows"), None)
    tiled = P(("groups", "rows"), None)
    return jax.shard_map(
        functools.partial(per_device, mesh.shape["rows"]),
        mesh=mesh,
        in_specs=(banded, tiled, tiled, P(), P(), P(), P()),
        out_specs=banded,
        check_vma=False,
    )
```

```python
import functools

import jax
import jax.numpy as jnp
from jax import lax
from jax.experimental import pallas as pl
from jax.experimental.pallas import tpu as pltpu
from jax.sharding import PartitionSpec as P

LAYERS = 3
TILE = 8
STAINS = 4
REACH = 2**LAYERS - 1
EPSILON = 1e-05
MESH = pl.DeviceIdType.MESH


def kernel(
    peers,
    slide_ref,
    flags_ref,
    index_ref,
    stain_ref,
    weights_ref,
    gain_ref,
    bias_ref,
    out_ref,
    slide,
    weights,
    result,
    turned,
    x0,
    x1,
    x2,
    response,
    taps,
    masks,
    flag_out,
    flag_in,
    tally_out,
    tally_in,
    edge_send,
    edge_recv,
    tally_send,
    tally_recv,
    local_sem,
):
    channels, rows, cols = slide_ref.shape
    tiles = flags_ref.shape[1]
    me = lax.axis_index("rows")
    has_up = me > 0
    has_down = me < peers - 1
    inputs = (x0, x1, x2)
    first = (REACH, REACH - 1, REACH - 3)
    base = REACH - 1

    flag_in[...] = jnp.zeros_like(flag_in)
    barrier = pltpu.get_barrier_semaphore()

    def greet(step, carry):
        other = lax.rem(me + step, peers)
        pl.semaphore_signal(barrier, inc=1, device_id={"rows": other}, device_id_type=MESH)
        return carry

    lax.fori_loop(1, peers, greet, 0)
    slide_copy = pltpu.make_async_copy(slide_ref, slide, local_sem.at[0])
    slide_copy.start()
    weights_copy = pltpu.make_async_copy(weights_ref, weights, local_sem.at[1])
    weights_copy.start()

    def loop(count, one):
        width = 2 if count % 2 == 0 else 1

        def several(step, carry):
            for k in range(width):
                one(step * width + k)
            return carry

        lax.fori_loop(0, count // width, several, 0)

    spread = (
        lax.broadcasted_iota(jnp.int32, (128, cols), 1) // TILE
        == lax.broadcasted_iota(jnp.int32, (128, cols), 0)
    ).astype(jnp.float32)
    eye = lax.broadcasted_iota(jnp.int32, (channels, channels), 0) == lax.broadcasted_iota(
        jnp.int32, (channels, channels), 1
    )

    def column(row):
        return jnp.sum(jnp.where(eye, row, 0.0), axis=1, keepdims=True)

    def as_row(col):
        return jnp.sum(jnp.where(eye, col, 0.0), axis=0, keepdims=True)

    def widen(flags):
        return jnp.dot(flags, spread, preferred_element_type=jnp.float32)

    flag_out[...] = jnp.zeros_like(flag_out)
    flag_out[:, 0:tiles] = jnp.broadcast_to(
        flags_ref[...].astype(jnp.float32), (flag_out.shape[0], tiles)
    )
    masks[0] = widen(flag_out[...])
    classes = jnp.dot(
        jnp.broadcast_to(index_ref[...].astype(jnp.float32), (8, tiles)),
        spread[0:tiles],
        preferred_element_type=jnp.float32,
    )[0:1]
    scale = jnp.zeros((channels, cols), jnp.float32)
    for stain in range(STAINS):
        scale = jnp.where(classes == stain, column(stain_ref[stain : stain + 1, :]), scale)

    chunks = cols // 128
    slide_copy.wait()
    for at in range(chunks):
        turned[at] = (
            slide[:, :, at * 128 : (at + 1) * 128]
            .astype(jnp.float32)
            .reshape(channels * rows, 128)
        )
    response[0] = scale
    lane = lax.broadcasted_iota(jnp.int32, (1, cols), 1)

    def place(buffer, row, values, spacing):
        buffer[1, row] = values.astype(jnp.bfloat16)
        shifted = pltpu.roll(values, spacing, 1)
        buffer[0, row] = jnp.where(lane >= spacing, shifted, 0.0).astype(jnp.bfloat16)
        shifted = pltpu.roll(values, cols - spacing, 1)
        buffer[2, row] = jnp.where(lane < cols - spacing, shifted, 0.0).astype(jnp.bfloat16)

    def load_row(row):
        values = jnp.concatenate(
            [turned[at, pl.ds(row, channels, stride=rows), :] for at in range(chunks)], axis=1
        )
        values = values * response[0] * masks[0, 0:1, :]
        values = values.astype(jnp.bfloat16).astype(jnp.float32)
        place(x0, first[0] + row, values, 1)

    loop(rows, load_row)

    @pl.when(jnp.logical_not(has_up))
    def _():
        x0[1, 0:REACH] = jnp.zeros((REACH, channels, cols), jnp.bfloat16)

    @pl.when(jnp.logical_not(has_down))
    def _():
        x0[1, REACH + rows : 2 * REACH + rows] = jnp.zeros((REACH, channels, cols), jnp.bfloat16)

    pl.semaphore_wait(barrier, peers - 1)

    def edge_copy(piece, side):
        if piece == 0:
            source, target = flag_out, flag_in.at[1 - side]
        else:
            lo, count = 2 ** (piece - 1) - 1, 2 ** (piece - 1)
            if side == 0:
                start, land = REACH + lo, REACH + rows + lo
            else:
                start, land = REACH + rows - lo - count, REACH - lo - count
            source, target = x0.at[1, pl.ds(start, count)], x0.at[1, pl.ds(land, count)]
        return pltpu.make_async_remote_copy(
            src_ref=source,
            dst_ref=target,
            send_sem=edge_send.at[piece, side],
            recv_sem=edge_recv.at[piece, side],
            device_id={"rows": me - 1 if side == 0 else me + 1},
            device_id_type=MESH,
        )

    def send_edge(piece):
        @pl.when(has_up)
        def _():
            edge_copy(piece, 0).start()

        @pl.when(has_down)
        def _():
            edge_copy(piece, 1).start()

    def take_edge(piece):
        @pl.when(has_down)
        def _():
            edge_copy(piece, 0).wait_recv()

        @pl.when(has_up)
        def _():
            edge_copy(piece, 1).wait_recv()

    for piece in (1, 0, 2):
        send_edge(piece)

    weights_copy.wait()
    for layer in range(LAYERS):
        for tap in range(9):
            taps[layer, :, tap * channels : (tap + 1) * channels] = weights[layer, tap]

    def widen_edge(piece):
        lo, count = 2 ** (piece - 1) - 1, 2 ** (piece - 1)
        for start in (REACH - lo - count, REACH + rows + lo):
            loop(count, lambda row: place_shifts(x0, start + row))

    def place_shifts(buffer, row):
        values = buffer[1, row].astype(jnp.float32)
        shifted = pltpu.roll(values, 1, 1)
        buffer[0, row] = jnp.where(lane >= 1, shifted, 0.0).astype(jnp.bfloat16)
        shifted = pltpu.roll(values, cols - 1, 1)
        buffer[2, row] = jnp.where(lane < cols - 1, shifted, 0.0).astype(jnp.bfloat16)

    def conv_row(layer, row):
        spacing = 2**layer
        source = inputs[layer]
        window = jnp.concatenate(
            [
                source[b, first[layer] + row + (a - 1) * spacing]
                for a in range(3)
                for b in range(3)
            ],
            axis=0,
        )
        return jnp.dot(taps[layer], window, preferred_element_type=jnp.float32)

    def conv_edges(layer, lo, count):
        for start in (-lo - count, rows + lo):

            def one(row):
                response[base + start + row] = conv_row(layer, start + row)

            loop(count, one)

    def fold(values):
        total = values[:, 0:128]
        for at in range(128, cols, 128):
            total = total + values[:, at : at + 128]
        return total

    def own_row(layer, row, carry):
        sums, squares = carry
        own = conv_row(layer, row)
        response[base + row] = own
        masked = own * masks[0, 0:1, :]
        return sums + fold(masked), squares + fold(masked * own)

    def own_rows(layer, start, count, carry):
        def two(step, carry):
            for k in range(2):
                carry = own_row(layer, start + 2 * step + k, carry)
            return carry

        return lax.fori_loop(0, count // 2, two, carry)

    def tally(layer, carry):
        sums, squares = carry
        tally_out[layer] = jnp.zeros(tally_out.shape[1:], jnp.float32)
        tally_out[layer, 0:1, 0:channels] = as_row(jnp.sum(sums, axis=1, keepdims=True))
        tally_out[layer, 1:2, 0:channels] = as_row(jnp.sum(squares, axis=1, keepdims=True))
        pixels = jnp.sum(masks[0, 0:1, :], axis=1, keepdims=True) * rows
        tally_out[layer, 2:3, :] = jnp.broadcast_to(pixels, (1, 128))
        tally_in[layer, me] = tally_out[layer]

    def tally_copy(layer, step, other, slot):
        return pltpu.make_async_remote_copy(
            src_ref=tally_out.at[layer],
            dst_ref=tally_in.at[layer, slot],
            send_sem=tally_send.at[layer, step],
            recv_sem=tally_recv.at[layer, slot],
            device_id={"rows": other},
            device_id_type=MESH,
        )

    def send_tally(layer):
        def one(step, carry):
            tally_copy(layer, step, lax.rem(me + step, peers), me).start()
            return carry

        lax.fori_loop(1, peers, one, 0)

    def take_tally(layer):
        def one(step, carry):
            other = lax.rem(me + step, peers)
            tally_copy(layer, step, other, other).wait_recv()
            return carry

        lax.fori_loop(1, peers, one, 0)
        total = jnp.sum(tally_in[layer], axis=0)
        count = total[2:3, 0:channels]
        average = total[0:1, 0:channels] / count
        variance = jnp.maximum(total[1:2, 0:channels] / count - average * average, 0.0)
        factor = gain_ref[layer : layer + 1, :] * lax.rsqrt(variance + EPSILON)
        return column(average), column(factor), column(bias_ref[layer : layer + 1, :])

    def finish_row(row, norm, mask):
        average, factor, bias = norm
        scaled = (response[base + row] - average) * factor + bias
        return jnp.maximum(scaled, 0.0) * masks[mask, 0:1, :]

    def finish(layer, start, count, norm, mask):
        def one(row):
            place(
                inputs[layer + 1],
                first[layer + 1] + start + row,
                finish_row(start + row, norm, mask),
                2 ** (layer + 1),
            )

        loop(count, one)

    def finish_edges(layer, lo, count, norm):
        finish(layer, -lo - count, count, norm, 1)
        finish(layer, rows + lo, count, norm, 2)

    nothing = jnp.zeros((channels, 128), jnp.float32)
    nothing = (nothing, nothing)

    inner = own_rows(0, 1, rows - 2, nothing)
    take_edge(1)
    widen_edge(1)
    tally(0, own_row(0, rows - 1, own_row(0, 0, inner)))
    send_tally(0)
    send_edge(3)
    take_edge(0)
    masks[1] = widen(flag_in[0])
    masks[2] = widen(flag_in[1])
    take_edge(2)
    widen_edge(2)
    conv_edges(0, 0, 2)
    norm0 = take_tally(0)
    finish(0, 0, rows, norm0, 0)
    finish_edges(0, 0, 2, norm0)
    tally(1, own_rows(1, 0, rows, nothing))
    send_tally(1)
    take_edge(3)
    widen_edge(3)
    conv_edges(0, 2, 4)
    finish_edges(0, 2, 4, norm0)
    conv_edges(1, 0, 4)
    norm1 = take_tally(1)
    finish(1, 0, rows, norm1, 0)
    finish_edges(1, 0, 4, norm1)
    tally(2, own_rows(2, 0, rows, nothing))
    send_tally(2)
    norm2 = take_tally(2)

    def last(row):
        values = finish_row(row, norm2, 0)
        for at in range(chunks):
            turned[at, pl.ds(row, channels, stride=rows), :] = values[:, at * 128 : (at + 1) * 128]

    loop(rows, last)
    for at in range(chunks):
        result[:, :, at * 128 : (at + 1) * 128] = (
            turned[at].reshape(channels, rows, 128).astype(result.dtype)
        )
    result_copy = pltpu.make_async_copy(result, out_ref, local_sem.at[2])
    result_copy.start()

    for piece in range(4):
        @pl.when(has_up)
        def _():
            edge_copy(piece, 0).wait_send()

        @pl.when(has_down)
        def _():
            edge_copy(piece, 1).wait_send()

    for layer in range(LAYERS):
        def one(step, carry):
            tally_copy(layer, step, lax.rem(me + step, peers), me).wait_send()
            return carry

        lax.fori_loop(1, peers, one, 0)

    result_copy.wait()


def per_device(peers, *arrays):
    channels, rows, cols = arrays[0].shape
    assert rows == TILE and rows > REACH and arrays[1].shape[0] == 1
    f32, bf16 = jnp.float32, jnp.bfloat16
    vmem = pl.BlockSpec(memory_space=pltpu.VMEM)
    hbm = pl.BlockSpec(memory_space=pl.ANY)
    return pl.pallas_call(
        functools.partial(kernel, peers),
        out_shape=jax.ShapeDtypeStruct((channels, rows, cols), bf16),
        in_specs=[hbm, vmem, vmem, vmem, hbm, vmem, vmem],
        out_specs=hbm,
        scratch_shapes=[
            pltpu.VMEM((channels, rows, cols), bf16),
            pltpu.VMEM(arrays[4].shape, bf16),
            pltpu.VMEM((channels, rows, cols), bf16),
            pltpu.VMEM((cols // 128, channels * rows, 128), f32),
            pltpu.VMEM((3, rows + 2 * REACH, channels, cols), bf16),
            pltpu.VMEM((3, rows + 2 * (REACH - 1), channels, cols), bf16),
            pltpu.VMEM((3, rows + 2 * (REACH - 3), channels, cols), bf16),
            pltpu.VMEM((rows + 2 * (REACH - 1), channels, cols), f32),
            pltpu.VMEM((LAYERS, channels, 9 * channels), bf16),
            pltpu.VMEM((3, 8, cols), f32),
            pltpu.VMEM((8, 128), f32),
            pltpu.VMEM((2, 8, 128), f32),
            pltpu.VMEM((LAYERS, 8, 128), f32),
            pltpu.VMEM((LAYERS, peers, 8, 128), f32),
            pltpu.SemaphoreType.DMA((4, 2)),
            pltpu.SemaphoreType.DMA((4, 2)),
            pltpu.SemaphoreType.DMA((LAYERS, peers)),
            pltpu.SemaphoreType.DMA((LAYERS, peers)),
            pltpu.SemaphoreType.DMA((3,)),
        ],
        compiler_params=pltpu.CompilerParams(
            collective_id=0, has_side_effects=True, vmem_limit_bytes=56 * 2**20
        ),
    )(*arrays)


def solution(mesh):
    banded = P(None, ("groups", "rows"), None)
    tiled = P(("groups", "rows"), None)
    return jax.shard_map(
        functools.partial(per_device, mesh.shape["rows"]),
        mesh=mesh,
        in_specs=(banded, tiled, tiled, P(), P(), P(), P()),
        out_specs=banded,
        check_vma=False,
    )
```

```python
import functools

import jax
import jax.numpy as jnp
from jax import lax
from jax.experimental import pallas as pl
from jax.experimental.pallas import tpu as pltpu
from jax.sharding import PartitionSpec as P

LAYERS = 3
TILE = 8
STAINS = 4
REACH = 2**LAYERS - 1
EPSILON = 1e-05
MESH = pl.DeviceIdType.MESH


def kernel(
    peers,
    slide_ref,
    flags_ref,
    index_ref,
    stain_ref,
    weights_ref,
    gain_ref,
    bias_ref,
    out_ref,
    slide,
    weights,
    result,
    turned,
    x0,
    x1,
    x2,
    response,
    taps,
    masks,
    flag_out,
    flag_in,
    tally_out,
    tally_in,
    edge_send,
    edge_recv,
    tally_send,
    tally_recv,
    local_sem,
):
    channels, rows, cols = slide_ref.shape
    tiles = flags_ref.shape[1]
    me = lax.axis_index("rows")
    has_up = me > 0
    has_down = me < peers - 1
    inputs = (x0, x1, x2)
    first = (REACH, REACH - 1, REACH - 3)
    base = REACH - 1

    flag_in[...] = jnp.zeros_like(flag_in)
    barrier = pltpu.get_barrier_semaphore()

    def greet(step, carry):
        other = lax.rem(me + step, peers)
        pl.semaphore_signal(barrier, inc=1, device_id={"rows": other}, device_id_type=MESH)
        return carry

    lax.fori_loop(1, peers, greet, 0)
    slide_copy = pltpu.make_async_copy(slide_ref, slide, local_sem.at[0])
    slide_copy.start()
    weights_copy = pltpu.make_async_copy(weights_ref, weights, local_sem.at[1])
    weights_copy.start()

    def loop(count, one):
        width = 2 if count % 2 == 0 else 1

        def several(step, carry):
            for k in range(width):
                one(step * width + k)
            return carry

        lax.fori_loop(0, count // width, several, 0)

    spread = (
        lax.broadcasted_iota(jnp.int32, (128, cols), 1) // TILE
        == lax.broadcasted_iota(jnp.int32, (128, cols), 0)
    ).astype(jnp.float32)
    eye = lax.broadcasted_iota(jnp.int32, (channels, channels), 0) == lax.broadcasted_iota(
        jnp.int32, (channels, channels), 1
    )

    def column(row):
        return jnp.sum(jnp.where(eye, row, 0.0), axis=1, keepdims=True)

    def as_row(col):
        return jnp.sum(jnp.where(eye, col, 0.0), axis=0, keepdims=True)

    def widen(flags):
        return jnp.dot(flags, spread, preferred_element_type=jnp.float32)

    flag_out[...] = jnp.zeros_like(flag_out)
    flag_out[:, 0:tiles] = jnp.broadcast_to(
        flags_ref[...].astype(jnp.float32), (flag_out.shape[0], tiles)
    )
    masks[0] = widen(flag_out[...])
    classes = jnp.dot(
        jnp.broadcast_to(index_ref[...].astype(jnp.float32), (8, tiles)),
        spread[0:tiles],
        preferred_element_type=jnp.float32,
    )[0:1]
    scale = jnp.zeros((channels, cols), jnp.float32)
    for stain in range(STAINS):
        scale = jnp.where(classes == stain, column(stain_ref[stain : stain + 1, :]), scale)

    chunks = cols // 128
    slide_copy.wait()
    for at in range(chunks):
        turned[at] = (
            slide[:, :, at * 128 : (at + 1) * 128]
            .astype(jnp.float32)
            .reshape(channels * rows, 128)
        )
    response[0] = scale
    lane = lax.broadcasted_iota(jnp.int32, (1, cols), 1)

    def place(buffer, row, values, spacing):
        buffer[1, row] = values.astype(jnp.bfloat16)
        shifted = pltpu.roll(values, spacing, 1)
        buffer[0, row] = jnp.where(lane >= spacing, shifted, 0.0).astype(jnp.bfloat16)
        shifted = pltpu.roll(values, cols - spacing, 1)
        buffer[2, row] = jnp.where(lane < cols - spacing, shifted, 0.0).astype(jnp.bfloat16)

    def load_row(row):
        values = jnp.concatenate(
            [turned[at, pl.ds(row, channels, stride=rows), :] for at in range(chunks)], axis=1
        )
        values = values * response[0] * masks[0, 0:1, :]
        values = values.astype(jnp.bfloat16).astype(jnp.float32)
        place(x0, first[0] + row, values, 1)

    loop(rows, load_row)

    @pl.when(jnp.logical_not(has_up))
    def _():
        x0[1, 0:REACH] = jnp.zeros((REACH, channels, cols), jnp.bfloat16)

    @pl.when(jnp.logical_not(has_down))
    def _():
        x0[1, REACH + rows : 2 * REACH + rows] = jnp.zeros((REACH, channels, cols), jnp.bfloat16)

    pl.semaphore_wait(barrier, peers - 1)

    pieces = {1: (0, 1), 2: (1, 2), 3: (3, 2), 4: (5, 2)}

    def edge_copy(piece, side):
        if piece == 0:
            source, target = flag_out, flag_in.at[1 - side]
        else:
            lo, count = pieces[piece]
            if side == 0:
                start, land = REACH + lo, REACH + rows + lo
            else:
                start, land = REACH + rows - lo - count, REACH - lo - count
            source, target = x0.at[1, pl.ds(start, count)], x0.at[1, pl.ds(land, count)]
        return pltpu.make_async_remote_copy(
            src_ref=source,
            dst_ref=target,
            send_sem=edge_send.at[piece, side],
            recv_sem=edge_recv.at[piece, side],
            device_id={"rows": me - 1 if side == 0 else me + 1},
            device_id_type=MESH,
        )

    def send_edge(piece):
        @pl.when(has_up)
        def _():
            edge_copy(piece, 0).start()

        @pl.when(has_down)
        def _():
            edge_copy(piece, 1).start()

    def take_edge(piece):
        @pl.when(has_down)
        def _():
            edge_copy(piece, 0).wait_recv()

        @pl.when(has_up)
        def _():
            edge_copy(piece, 1).wait_recv()

    for piece in (1, 0, 2):
        send_edge(piece)

    weights_copy.wait()
    for layer in range(LAYERS):
        for tap in range(9):
            taps[layer, :, tap * channels : (tap + 1) * channels] = weights[layer, tap]

    def widen_edge(piece):
        lo, count = pieces[piece]
        for start in (REACH - lo - count, REACH + rows + lo):
            loop(count, lambda row: place_shifts(x0, start + row))

    def place_shifts(buffer, row):
        values = buffer[1, row].astype(jnp.float32)
        shifted = pltpu.roll(values, 1, 1)
        buffer[0, row] = jnp.where(lane >= 1, shifted, 0.0).astype(jnp.bfloat16)
        shifted = pltpu.roll(values, cols - 1, 1)
        buffer[2, row] = jnp.where(lane < cols - 1, shifted, 0.0).astype(jnp.bfloat16)

    def conv_row(layer, row):
        spacing = 2**layer
        source = inputs[layer]
        window = jnp.concatenate(
            [
                source[b, first[layer] + row + (a - 1) * spacing]
                for a in range(3)
                for b in range(3)
            ],
            axis=0,
        )
        return jnp.dot(taps[layer], window, preferred_element_type=jnp.float32)

    def conv_edges(layer, lo, count):
        for start in (-lo - count, rows + lo):

            def one(row):
                response[base + start + row] = conv_row(layer, start + row)

            loop(count, one)

    def fold(values):
        total = values[:, 0:128]
        for at in range(128, cols, 128):
            total = total + values[:, at : at + 128]
        return total

    def own_row(layer, row, carry):
        sums, squares = carry
        own = conv_row(layer, row)
        response[base + row] = own
        masked = own * masks[0, 0:1, :]
        return sums + fold(masked), squares + fold(masked * own)

    def own_rows(layer, start, count, carry):
        def two(step, carry):
            for k in range(2):
                carry = own_row(layer, start + 2 * step + k, carry)
            return carry

        return lax.fori_loop(0, count // 2, two, carry)

    def tally(layer, carry):
        sums, squares = carry
        tally_out[layer, 0:1, 0:channels] = as_row(jnp.sum(sums, axis=1, keepdims=True))
        tally_out[layer, 1:2, 0:channels] = as_row(jnp.sum(squares, axis=1, keepdims=True))
        pixels = jnp.sum(masks[0, 0:1, :], axis=1, keepdims=True) * rows
        tally_out[layer, :, channels:] = jnp.broadcast_to(pixels, (2, 128 - channels))
        tally_in[layer, me] = tally_out[layer]

    def tally_copy(layer, step, other, slot):
        return pltpu.make_async_remote_copy(
            src_ref=tally_out.at[layer],
            dst_ref=tally_in.at[layer, slot],
            send_sem=tally_send.at[layer, step],
            recv_sem=tally_recv.at[layer, slot],
            device_id={"rows": other},
            device_id_type=MESH,
        )

    def send_tally(layer):
        def one(turn, carry):
            step = peers - turn

            @pl.when(me + step < peers)
            def _():
                tally_copy(layer, step, me + step, me).start()

            @pl.when(me >= step)
            def _():
                tally_copy(layer, peers - step, me - step, me).start()

            return carry

        lax.fori_loop(1, peers, one, 0)

    def take_tally(layer):
        def one(step, carry):
            other = lax.rem(me + step, peers)
            tally_copy(layer, step, other, other).wait_recv()
            return carry

        lax.fori_loop(1, peers, one, 0)
        total = jnp.sum(tally_in[layer], axis=0)
        count = total[0:1, channels : channels + 1]
        average = total[0:1, 0:channels] / count
        variance = jnp.maximum(total[1:2, 0:channels] / count - average * average, 0.0)
        factor = gain_ref[layer : layer + 1, :] * lax.rsqrt(variance + EPSILON)
        return column(average), column(factor), column(bias_ref[layer : layer + 1, :])

    def finish_row(row, norm, mask):
        average, factor, bias = norm
        scaled = (response[base + row] - average) * factor + bias
        return jnp.maximum(scaled, 0.0) * masks[mask, 0:1, :]

    def finish(layer, start, count, norm, mask):
        def one(row):
            place(
                inputs[layer + 1],
                first[layer + 1] + start + row,
                finish_row(start + row, norm, mask),
                2 ** (layer + 1),
            )

        loop(count, one)

    def finish_edges(layer, lo, count, norm):
        finish(layer, -lo - count, count, norm, 1)
        finish(layer, rows + lo, count, norm, 2)

    nothing = jnp.zeros((channels, 128), jnp.float32)
    nothing = (nothing, nothing)

    inner = own_rows(0, 1, rows - 2, nothing)
    take_edge(1)
    widen_edge(1)
    tally(0, own_row(0, rows - 1, own_row(0, 0, inner)))
    send_tally(0)
    send_edge(3)
    send_edge(4)
    take_edge(0)
    masks[1] = widen(flag_in[0])
    masks[2] = widen(flag_in[1])
    take_edge(2)
    widen_edge(2)
    conv_edges(0, 0, 2)
    norm0 = take_tally(0)
    finish(0, 0, rows, norm0, 0)
    finish_edges(0, 0, 2, norm0)
    tally(1, own_rows(1, 0, rows, nothing))
    send_tally(1)
    for piece, lo in ((3, 2), (4, 4)):
        take_edge(piece)
        widen_edge(piece)
        conv_edges(0, lo, 2)
        finish_edges(0, lo, 2, norm0)
        conv_edges(1, lo - 2, 2)
    norm1 = take_tally(1)
    finish(1, 0, rows, norm1, 0)
    finish_edges(1, 0, 4, norm1)
    tally(2, own_rows(2, 0, rows, nothing))
    send_tally(2)
    norm2 = take_tally(2)

    def last(row):
        values = finish_row(row, norm2, 0)
        for at in range(chunks):
            turned[at, pl.ds(row, channels, stride=rows), :] = values[:, at * 128 : (at + 1) * 128]

    loop(rows, last)
    for at in range(chunks):
        result[:, :, at * 128 : (at + 1) * 128] = (
            turned[at].reshape(channels, rows, 128).astype(result.dtype)
        )
    result_copy = pltpu.make_async_copy(result, out_ref, local_sem.at[2])
    result_copy.start()

    for piece in range(5):
        @pl.when(has_up)
        def _():
            edge_copy(piece, 0).wait_send()

        @pl.when(has_down)
        def _():
            edge_copy(piece, 1).wait_send()

    for layer in range(LAYERS):
        def one(step, carry):
            tally_copy(layer, step, lax.rem(me + step, peers), me).wait_send()
            return carry

        lax.fori_loop(1, peers, one, 0)

    result_copy.wait()


def per_device(peers, *arrays):
    channels, rows, cols = arrays[0].shape
    assert rows == TILE and rows > REACH and arrays[1].shape[0] == 1 and channels < 128
    f32, bf16 = jnp.float32, jnp.bfloat16
    vmem = pl.BlockSpec(memory_space=pltpu.VMEM)
    hbm = pl.BlockSpec(memory_space=pl.ANY)
    return pl.pallas_call(
        functools.partial(kernel, peers),
        out_shape=jax.ShapeDtypeStruct((channels, rows, cols), bf16),
        in_specs=[hbm, vmem, vmem, vmem, hbm, vmem, vmem],
        out_specs=hbm,
        scratch_shapes=[
            pltpu.VMEM((channels, rows, cols), bf16),
            pltpu.VMEM(arrays[4].shape, bf16),
            pltpu.VMEM((channels, rows, cols), bf16),
            pltpu.VMEM((cols // 128, channels * rows, 128), f32),
            pltpu.VMEM((3, rows + 2 * REACH, channels, cols), bf16),
            pltpu.VMEM((3, rows + 2 * (REACH - 1), channels, cols), bf16),
            pltpu.VMEM((3, rows + 2 * (REACH - 3), channels, cols), bf16),
            pltpu.VMEM((rows + 2 * (REACH - 1), channels, cols), f32),
            pltpu.VMEM((LAYERS, channels, 9 * channels), bf16),
            pltpu.VMEM((3, 8, cols), f32),
            pltpu.VMEM((8, 128), f32),
            pltpu.VMEM((2, 8, 128), f32),
            pltpu.VMEM((LAYERS, 2, 128), f32),
            pltpu.VMEM((LAYERS, peers, 2, 128), f32),
            pltpu.SemaphoreType.DMA((5, 2)),
            pltpu.SemaphoreType.DMA((5, 2)),
            pltpu.SemaphoreType.DMA((LAYERS, peers)),
            pltpu.SemaphoreType.DMA((LAYERS, peers)),
            pltpu.SemaphoreType.DMA((3,)),
        ],
        compiler_params=pltpu.CompilerParams(
            collective_id=0, has_side_effects=True, vmem_limit_bytes=56 * 2**20
        ),
    )(*arrays)


def solution(mesh):
    banded = P(None, ("groups", "rows"), None)
    tiled = P(("groups", "rows"), None)
    return jax.shard_map(
        functools.partial(per_device, mesh.shape["rows"]),
        mesh=mesh,
        in_specs=(banded, tiled, tiled, P(), P(), P(), P()),
        out_specs=banded,
        check_vma=False,
    )
```
